32 devices in a mesh: dp: 8 (over y, x, core), seq: 4 (over z).
Axes of the slice: x: 2, y: 2, z: 4, core: 2. Of those that a mesh axis runs over, the one named last changes fastest.
Arguments:
- hidden_in: bfloat16 [8, 512, 2048], P('dp', 'seq'), may hold values from -6 to 6
- cotangent: bfloat16 [8, 512, 2048], P('dp', 'seq'), may hold values from -6 to 6
- norm_gain: float32 [2048], P('dp'), may hold values from 0.1 to 1.9
- route_weights: float32 [8, 512, 10], P('dp', 'seq'), may hold values from 0.1 to 1
- expert_ids: int32 [8, 512, 10], P('dp', 'seq'), may hold values from 0 to 63, all different within a row; in each aligned block of 128 rows (0 to 127, 128 to 255, ..., all dimensions but the last counted through in order) at most 24 rows name the same one
- expert_gate: bfloat16 [64, 2048, 512], P(('dp', 'seq')), may hold values from -0.125 to 0.125
- expert_up: bfloat16 [64, 2048, 512], P(('dp', 'seq')), may hold values from -0.125 to 0.125
- expert_down: bfloat16 [64, 512, 2048], P(('dp', 'seq')), may hold values from -0.25 to 0.25
Outputs:
- grad_hidden: bfloat16 [8, 512, 2048], P('dp', 'seq')
- grad_gain: float32 [2048], P('dp')
- grad_gate: bfloat16 [64, 2048, 512], P(('dp', 'seq'))
- grad_up: bfloat16 [64, 2048, 512], P(('dp', 'seq'))
- grad_down: bfloat16 [64, 512, 2048], P(('dp', 'seq'))
The draws below stay inside these ranges and needn't reach their ends.
Inputs may be any that keep to these rules, and one draw needn't show every extreme that they name: `expert_ids`: each token names 10 different experts. Among the rows of one device no expert is named by more than 24 of them, and in some device one expert is named by exactly 24.
All inputs are finite; a program needn't handle non-finite values.
Results may differ from the reference program's by a relative error of at most 0.0072.
Values may be sent and summed in bfloat16 or wider, within the bound.
A program may use at most 192 MiB of HBM per device.

```python
import math
import jax
import jax.numpy as jnp
import numpy as np
from jax import lax

D = 2048
HIDDEN_SIZE = 512
TOP = 10
TOK_DEV = 128
SEQS = 8
LEN = 512
EXPERTS = 64
CAP = 24
N_DP = 8
N_SEQ = 4


def block_scale(key, dims, pieces, least, high):
    level = 1.0
    for axis_at, shards_of in pieces:
        draws = jax.random.uniform(jax.random.fold_in(jax.random.fold_in(key, 6), axis_at), (shards_of,), jnp.float32, least / len(pieces), high / len(pieces))
        level = level * jnp.repeat(jnp.exp(draws), dims[axis_at] // shards_of).reshape((-1,) + (1,) * (len(dims) - 1 - axis_at))
    return level


def shared_out(key, own, number, rows, amount, top, reach, slope):
    order = jax.random.permutation(key, amount)
    heavy_load, ordinary = portions_of(amount, rows * top, reach, slope, True), portions_of(amount, rows * top, reach, slope, False)
    places = jnp.arange(amount)

    def named(lengths, rotation):
        used = int((lengths > 0).sum())
        fixed = max(1, used // 4)
        shifted = fixed + (places - fixed + rotation * (used - fixed)) % max(1, amount - fixed)
        return jnp.zeros((amount,), jnp.int32).at[order[jnp.where(places < fixed, places, shifted)]].set(jnp.asarray(lengths, jnp.int32))

    lengths = jnp.where(number % 4 == 0, named(heavy_load, number // 4), named(ordinary, number - number // 4 - 1))
    mixed = jax.random.permutation(jax.random.fold_in(own, 3), amount)
    giver, sink = mixed[0:amount // 2 * 2:2], mixed[1:amount // 2 * 2:2]
    room = jnp.minimum(lengths[giver] - 1, reach - lengths[sink]) // 2
    room = jnp.where((giver == order[0]) | (sink == order[0]) | (lengths[sink] == 0), 0, jnp.maximum(room, 0))
    shifted = jax.random.randint(jax.random.fold_in(own, 4), (amount // 2,), 0, 1 << 20) % (room + 1)
    lengths = lengths.at[giver].add(-shifted).at[sink].add(shifted)
    members = jnp.searchsorted(jnp.cumsum(lengths), jnp.arange(rows * top), side="right").astype(jnp.int32)
    grid = members.reshape(top, rows).T
    grid = grid[jax.random.permutation(jax.random.fold_in(own, 1), rows)]
    rotation = jax.random.randint(jax.random.fold_in(own, 2), (rows, 1), 0, top)
    return jnp.take_along_axis(grid, (jnp.arange(top)[None, :] + rotation) % top, axis=1)


def portions_of(count, total, limit, skew, full):
    portions = [(1 << 20) // math.isqrt(rank ** skew) + 1 for rank in range(1, count + 1)]
    largest = limit if full else min(limit, max(-(-total // count), total * portions[0] // sum(portions)))
    least = 1 if total - largest >= count - 1 else 0
    given, rest = [largest] + [least] * (count - 1), total - largest - least * (count - 1)
    while rest > 0:
        candidates = [i for i in range(1, count) if given[i] < largest] or [i for i in range(1, count) if given[i] < limit]
        whole, left = sum([portions[i] for i in candidates]), rest
        for i in candidates:
            addition = min(limit - given[i], max(1, left * portions[i] // whole), rest)
            given[i] = given[i] + addition
            rest = rest - addition
    return np.array(given)


def normal_values(rng, shape, spread, bound, cuts=(), kind=jnp.bfloat16):
    array = jax.random.normal(rng, shape, jnp.float32) * spread
    if len(cuts) > 0:
        array = block_scale(rng, shape, cuts, -0.22, 0.18) * array
    return jnp.clip(array, min=-bound, max=bound).astype(kind)


def setup_inputs(seed: int = 0) -> dict:
    key_list = jax.random.split(jax.random.key(seed), 9)
    hidden_in = normal_values(key_list[0], (SEQS, LEN, D), 1.0, 6.0, ((0, 8), (1, 4)))
    cotangent = normal_values(key_list[1], (SEQS, LEN, D), 1.0, 6.0, ((0, 8), (1, 4)))
    norm_gain = jnp.clip(1.0 + 0.18 * jax.random.normal(key_list[2], (D,), jnp.float32), 0.1, 1.9)
    route_weights = jnp.clip(jnp.exp(math.log(1.0) - 2.3025851 * jax.random.uniform(key_list[3], (SEQS, LEN, TOP), jnp.float32) ** block_scale(key_list[3], (SEQS, LEN, TOP), ((0, 8), (1, 4)), -0.2, 0.2)), 0.1, 1.0)
    expert_ids_keys = jax.random.split(jax.random.fold_in(key_list[4], 1), SEQS * LEN // TOK_DEV)
    expert_ids_turns = jax.random.permutation(jax.random.fold_in(key_list[4], 3), SEQS * LEN // TOK_DEV)
    expert_ids = jax.vmap(lambda own, number: shared_out(jax.random.fold_in(key_list[4], 2), own, number, TOK_DEV, EXPERTS, TOP, CAP, 2))(expert_ids_keys, expert_ids_turns).reshape((SEQS, LEN, TOP))
    expert_gate = normal_values(key_list[5], (EXPERTS, D, HIDDEN_SIZE), D ** -0.5, 0.125, ((0, 32),))
    expert_up = normal_values(key_list[6], (EXPERTS, D, HIDDEN_SIZE), D ** -0.5, 0.125, ((0, 32),))
    expert_down = normal_values(key_list[7], (EXPERTS, HIDDEN_SIZE, D), HIDDEN_SIZE ** -0.5, 0.25, ((0, 32),))
    return dict(hidden_in=hidden_in, cotangent=cotangent, norm_gain=norm_gain, route_weights=route_weights, expert_ids=expert_ids, expert_gate=expert_gate, expert_up=expert_up, expert_down=expert_down)


EPSILON = 1e-06

def block_slots(block_experts):
    flat_experts = block_experts.reshape(-1)
    onehot = (flat_experts[:, None] == jnp.arange(EXPERTS, dtype=jnp.int32)[None, :]).astype(jnp.float32)
    before = jnp.cumsum(onehot, axis=0) - onehot
    earlier_count = lax.optimization_barrier(jnp.sum(before * onehot, axis=1)).astype(jnp.int32)
    return flat_experts * CAP + earlier_count

def reference(hidden_in, cotangent, norm_gain, route_weights, expert_ids, expert_gate, expert_up, expert_down):
    blocks = N_DP * N_SEQ
    model_width = hidden_in.shape[-1]
    per_block = TOK_DEV * TOP
    inputs = hidden_in.reshape(blocks * TOK_DEV, model_width).astype(jnp.float32)
    inverse_root = lax.rsqrt(lax.optimization_barrier(jnp.mean(inputs * inputs, axis=1, keepdims=True)) + EPSILON)
    scaled = inputs * inverse_root
    normed = (scaled * norm_gain[None, :]).astype(jnp.bfloat16)
    upstream = cotangent.reshape(blocks * TOK_DEV, model_width)
    weights_flat = route_weights.reshape(blocks * per_block)
    slot_index = lax.map(block_slots, expert_ids.reshape(blocks, TOK_DEV, TOP))

    def fill_table(block_slot):
        return jnp.zeros((EXPERTS * CAP,), jnp.int32).at[block_slot].set(jnp.arange(per_block, dtype=jnp.int32) + 1)
    slot_table = jax.vmap(fill_table)(slot_index)
    slot_table = slot_table.reshape(blocks, EXPERTS, CAP).transpose(1, 0, 2).reshape(EXPERTS, blocks * CAP)
    block_of_row = jnp.arange(blocks * CAP, dtype=jnp.int32) // CAP

    def one_expert(packed):
        slot_entry, gate_matrix, up_matrix, down_matrix = packed
        occupied = slot_entry > 0
        within = jnp.maximum(slot_entry - 1, 0)
        assignment = block_of_row * per_block + within
        token_row = block_of_row * TOK_DEV + within // TOP
        rows_in = jnp.where(occupied[:, None], normed[token_row], jnp.zeros((), jnp.bfloat16))
        row_weight = jnp.where(occupied, weights_flat[assignment], jnp.zeros((), jnp.float32))
        rows_grad = (row_weight[:, None] * upstream[token_row].astype(jnp.float32)).astype(jnp.bfloat16)
        pre_gate = jnp.dot(rows_in, gate_matrix, preferred_element_type=jnp.float32)
        pre_up = jnp.dot(rows_in, up_matrix, preferred_element_type=jnp.float32)
        sigmoid_gate = jax.nn.sigmoid(pre_gate)
        silu_gate = pre_gate * sigmoid_gate
        activation = (silu_gate * pre_up).astype(jnp.bfloat16)
        grad_act = jnp.dot(rows_grad, down_matrix.T, preferred_element_type=jnp.float32)
        gate_back = (grad_act * pre_up * sigmoid_gate * (1.0 + pre_gate * (1.0 - sigmoid_gate))).astype(jnp.bfloat16)
        up_back = (grad_act * silu_gate).astype(jnp.bfloat16)
        down_grad = jnp.dot(activation.T, rows_grad, preferred_element_type=jnp.float32).astype(jnp.bfloat16)
        gate_grad = jnp.dot(rows_in.T, gate_back, preferred_element_type=jnp.float32).astype(jnp.bfloat16)
        up_grad = jnp.dot(rows_in.T, up_back, preferred_element_type=jnp.float32).astype(jnp.bfloat16)
        returned = (jnp.dot(gate_back, gate_matrix.T, preferred_element_type=jnp.float32) + jnp.dot(up_back, up_matrix.T, preferred_element_type=jnp.float32)).astype(jnp.bfloat16)
        return (gate_grad, up_grad, down_grad, returned)
    grad_gate, grad_up, grad_down, returned = lax.map(one_expert, (slot_table, expert_gate, expert_up, expert_down))
    flat_back = returned.reshape(EXPERTS * blocks * CAP, model_width)

    def gather_block(packed):
        block_number, block_slot = packed
        where_rows = block_slot // CAP * (blocks * CAP) + block_number * CAP + block_slot % CAP
        picked = flat_back[where_rows].astype(jnp.float32).reshape(TOK_DEV, TOP, model_width)
        return lax.optimization_barrier(jnp.sum(picked, axis=1))
    summed = lax.map(gather_block, (jnp.arange(blocks, dtype=jnp.int32), slot_index))
    summed = summed.reshape(blocks * TOK_DEV, model_width)
    grad_gain = lax.optimization_barrier(jnp.sum(summed * scaled, axis=0))
    gained = summed * norm_gain[None, :]
    centered = lax.optimization_barrier(jnp.mean(gained * scaled, axis=1, keepdims=True))
    grad_hidden = (upstream.astype(jnp.float32) + inverse_root * (gained - scaled * centered)).astype(jnp.bfloat16)
    return (grad_hidden.reshape(hidden_in.shape), grad_gain, grad_gate, grad_up, grad_down)
```

```python
import functools

import jax
import jax.numpy as jnp
from jax import lax
from jax.experimental import pallas as pl
from jax.experimental.pallas import tpu as pltpu
from jax.sharding import PartitionSpec as P

TOP = 10


EPSILON = 1e-06


def flipped(index, bit):
    return index + (1 - 2 * ((index // (1 << bit)) % 2)) * (1 << bit)


def spread_kernel(dp_count, seq_count, count, orders, total_sends, *refs):
    ins, outs = refs[:count], refs[count : 2 * count]
    holds = refs[2 * count : 3 * count]
    send_sem, recv_sem, local_sem = refs[3 * count :]
    devices = dp_count * seq_count
    dp, z = lax.axis_index("dp"), lax.axis_index("seq")
    own = dp * seq_count + z
    pending = []

    def guarded(conds, action):
        if not conds:
            action()
            return
        whole = conds[0]
        for extra in conds[1:]:
            whole = jnp.logical_and(whole, extra)
        pl.when(whole)(action)

    def send(array, source, block, target_dp, target_z, conds):
        copy = pltpu.make_async_remote_copy(
            src_ref=source,
            dst_ref=outs[array].at[block],
            send_sem=send_sem.at[len(pending)],
            recv_sem=recv_sem.at[array * devices + block],
            device_id=(target_dp, target_z),
            device_id_type=pl.DeviceIdType.MESH,
        )
        guarded(conds, copy.start)
        pending.append((conds, copy))

    def fan_out(array, first, source, block, conds):
        for bit in orders[array][first:]:
            send(array, source, block, flipped(dp, bit), z, conds)

    def arrived(array, block, conds):
        copy = pltpu.make_async_remote_copy(
            src_ref=outs[array].at[block],
            dst_ref=outs[array].at[block],
            send_sem=send_sem.at[0],
            recv_sem=recv_sem.at[array * devices + block],
            device_id=(flipped(dp, 0), z),
            device_id_type=pl.DeviceIdType.MESH,
        )
        guarded(conds, copy.wait_recv)

    taken = [
        pltpu.make_async_copy(ins[a], holds[a], local_sem.at[2 * a]) for a in range(count)
    ]
    put = [
        pltpu.make_async_copy(holds[a], outs[a].at[own], local_sem.at[2 * a + 1])
        for a in range(count)
    ]
    for copy in taken:
        copy.start()
    for array in range(count):
        send(array, ins[array], own, dp, z + 1, [z + 1 < seq_count])
        send(array, ins[array], own, dp, z - 1, [z > 0])
        fan_out(array, 0, ins[array], own, [])
    for a in range(count):
        taken[a].wait()
        put[a].start()

    def line_round(step):
        for array in range(count):
            for way in (1, -1):
                origin = z - way * step
                there = [origin >= 0, origin < seq_count]
                block = dp * seq_count + origin
                arrived(array, block, there)
                source = outs[array].at[block]
                if step < seq_count - 1:
                    beyond = z + way
                    onward = there + [beyond >= 0, beyond < seq_count]
                    send(array, source, block, dp, beyond, onward)
                fan_out(array, 0, source, block, there)

    def bit_round(stage, step):
        for array in range(count):
            order = orders[array]
            for combo in range(1 << stage):
                origin_dp = flipped(dp, order[stage])
                for place in range(stage):
                    if (combo >> place) & 1:
                        origin_dp = flipped(origin_dp, order[place])
                for offset in (0,) if step == 0 else (-step, step):
                    origin = z + offset
                    there = [] if step == 0 else [origin >= 0, origin < seq_count]
                    block = origin_dp * seq_count + origin
                    arrived(array, block, there)
                    fan_out(array, stage + 1, outs[array].at[block], block, there)

    for step in range(1, seq_count):
        line_round(step)
        bit_round(0, step - 1)
    bit_round(0, seq_count - 1)
    for stage in range(1, len(orders[0])):
        for step in range(seq_count):
            bit_round(stage, step)
    for copy in put:
        copy.wait()
    for conds, copy in pending:
        guarded(conds, copy.wait_send)
    assert len(pending) == total_sends


def spread(arrays, dp_count, seq_count):
    count = len(arrays)
    devices = dp_count * seq_count
    bits = (dp_count - 1).bit_length()
    upward = tuple(range(1, bits)) + (0,)
    downward = tuple(range(bits - 1, 0, -1)) + (0,)
    orders = [downward if a % 2 else upward for a in range(count)]
    calls = 2 * seq_count - 1
    per_array = 2 * (seq_count - 1) + calls * ((1 << bits) - 1)
    anywhere = pl.BlockSpec(memory_space=pl.ANY)
    return pl.pallas_call(
        functools.partial(
            spread_kernel, dp_count, seq_count, count, orders, count * per_array
        ),
        out_shape=[jax.ShapeDtypeStruct((devices,) + a.shape, a.dtype) for a in arrays],
        in_specs=[anywhere] * count,
        out_specs=[anywhere] * count,
        scratch_shapes=[pltpu.VMEM(a.shape, a.dtype) for a in arrays]
        + [
            pltpu.SemaphoreType.DMA((count * per_array,)),
            pltpu.SemaphoreType.DMA((count * devices,)),
            pltpu.SemaphoreType.DMA((2 * count,)),
        ],
        compiler_params=pltpu.CompilerParams(
            has_side_effects=True, vmem_limit_bytes=16 * 1024 * 1024
        ),
        cost_estimate=pl.CostEstimate(flops=0, bytes_accessed=200_000_000, transcendentals=0),
    )(*arrays)


def shards(
    hidden_in, cotangent, norm_gain, route_weights, expert_ids, expert_gate, expert_up, expert_down
):
    tokens_here = hidden_in.shape[1]
    model_width = hidden_in.shape[2]
    local_experts = expert_gate.shape[0]
    dp_count = lax.axis_size("dp")
    seq_count = lax.axis_size("seq")
    devices = dp_count * seq_count
    expert_count = local_experts * devices
    capacity = max(2, tokens_here * TOP * 6 // (5 * expert_count))
    own_weights = route_weights[0].T
    own_ids = expert_ids[0].T
    gain_rows = norm_gain.shape[0] // tokens_here
    table = jnp.concatenate(
        [own_weights, own_ids.astype(jnp.float32), norm_gain.reshape(gain_rows, tokens_here)],
        axis=0,
    )
    table = jnp.pad(table, ((0, -table.shape[0] % 8), (0, 0)))
    all_tables, all_hidden, all_upstream = spread(
        (table, hidden_in[0], cotangent[0]), dp_count, seq_count
    )
    gain_full = all_tables.reshape(dp_count, seq_count, -1, tokens_here)[
        :, 0, 2 * TOP : 2 * TOP + gain_rows
    ].reshape(model_width)
    position = jnp.arange(tokens_here, dtype=jnp.int32)
    earlier = (position[:, None] < position[None, :]).astype(jnp.bfloat16)
    slots = jnp.arange(capacity, dtype=jnp.int32).astype(jnp.float32)

    my_device = lax.axis_index("dp") * seq_count + lax.axis_index("seq")
    mine = (my_device * local_experts + jnp.arange(local_experts, dtype=jnp.int32)).astype(
        jnp.float32
    )
    matches = all_tables[:, None, TOP : 2 * TOP, :] == mine[None, :, None, None]
    named = jnp.any(matches, axis=2)
    token_weight = jnp.sum(jnp.where(matches, all_tables[:, None, :TOP, :], 0.0), axis=2)
    before = jnp.einsum(
        "nit,tu->niu", named.astype(jnp.bfloat16), earlier, preferred_element_type=jnp.float32
    )
    chosen = named[:, :, None, :] & (before[:, :, None, :] == slots[None, None, :, None])
    pick = chosen.astype(jnp.bfloat16)
    row_weight = jnp.sum(jnp.where(chosen, token_weight[:, :, None, :], 0.0), axis=3)
    pick_flat = pick.reshape(devices, local_experts * capacity, tokens_here)
    four_shape = (devices, local_experts, capacity, model_width)

    picked = jnp.einsum(
        "nst,ntd->nsd", pick_flat, all_hidden, preferred_element_type=jnp.float32
    ).astype(jnp.bfloat16)
    picked32 = picked.astype(jnp.float32)
    picked_root = lax.rsqrt(jnp.mean(picked32 * picked32, axis=2, keepdims=True) + EPSILON)
    rows_in = (
        (picked32 * picked_root * gain_full[None, None, :])
        .astype(jnp.bfloat16)
        .reshape(four_shape)
    )
    rows_grad = (
        jnp.einsum("nst,ntd->nsd", pick_flat, all_upstream, preferred_element_type=jnp.float32)
        * row_weight.reshape(devices, local_experts * capacity)[:, :, None]
    ).astype(jnp.bfloat16).reshape(four_shape)

    pre_gate = jnp.einsum(
        "nicd,idf->nicf", rows_in, expert_gate, preferred_element_type=jnp.float32
    )
    pre_up = jnp.einsum("nicd,idf->nicf", rows_in, expert_up, preferred_element_type=jnp.float32)
    sigmoid_gate = jax.nn.sigmoid(pre_gate)
    silu_gate = pre_gate * sigmoid_gate
    activation = (silu_gate * pre_up).astype(jnp.bfloat16)
    grad_act = jnp.einsum(
        "nicd,ifd->nicf", rows_grad, expert_down, preferred_element_type=jnp.float32
    )
    gate_back = (grad_act * pre_up * sigmoid_gate * (1.0 + pre_gate * (1.0 - sigmoid_gate))).astype(
        jnp.bfloat16
    )
    up_back = (grad_act * silu_gate).astype(jnp.bfloat16)
    grad_down = jnp.einsum(
        "nicf,nicd->ifd", activation, rows_grad, preferred_element_type=jnp.float32
    ).astype(jnp.bfloat16)
    grad_gate = jnp.einsum(
        "nicd,nicf->idf", rows_in, gate_back, preferred_element_type=jnp.float32
    ).astype(jnp.bfloat16)
    grad_up = jnp.einsum(
        "nicd,nicf->idf", rows_in, up_back, preferred_element_type=jnp.float32
    ).astype(jnp.bfloat16)
    returned = (
        jnp.einsum("nicf,idf->nicd", gate_back, expert_gate, preferred_element_type=jnp.float32)
        + jnp.einsum("nicf,idf->nicd", up_back, expert_up, preferred_element_type=jnp.float32)
    ).astype(jnp.bfloat16)
    back_rows = lax.all_to_all(
        returned.reshape(devices, local_experts * capacity, model_width),
        ("dp", "seq"),
        split_axis=0,
        concat_axis=0,
        tiled=True,
    )
    back_flat = back_rows.reshape(expert_count * capacity, model_width)

    every = jnp.arange(expert_count, dtype=jnp.int32)
    own_named = jnp.any(own_ids[None, :, :] == every[:, None, None], axis=1)
    own_before = jnp.dot(
        own_named.astype(jnp.bfloat16), earlier, preferred_element_type=jnp.float32
    )
    own_pick = (
        (own_named[:, None, :] & (own_before[:, None, :] == slots[None, :, None]))
        .astype(jnp.bfloat16)
        .reshape(expert_count * capacity, tokens_here)
    )
    summed = jnp.einsum("st,sd->td", own_pick, back_flat, preferred_element_type=jnp.float32)

    inputs = hidden_in[0].astype(jnp.float32)
    upstream = cotangent[0]
    inverse_root = lax.rsqrt(jnp.mean(inputs * inputs, axis=1, keepdims=True) + EPSILON)
    scaled = inputs * inverse_root
    local_gain = jnp.sum(summed * scaled, axis=0)
    partial_share = lax.psum_scatter(local_gain, "dp", scatter_dimension=0, tiled=True)
    grad_gain = lax.psum(partial_share, "seq")
    gained = summed * gain_full[None, :]
    centered = jnp.mean(gained * scaled, axis=1, keepdims=True)
    grad_hidden = (
        upstream.astype(jnp.float32) + inverse_root * (gained - scaled * centered)
    ).astype(jnp.bfloat16)
    return (grad_hidden.reshape(hidden_in.shape), grad_gain, grad_gate, grad_up, grad_down)


def solution(mesh):
    return jax.shard_map(
        shards,
        mesh=mesh,
        in_specs=(
            P("dp", "seq", None),
            P("dp", "seq", None),
            P("dp"),
            P("dp", "seq", None),
            P("dp", "seq", None),
            P(("dp", "seq"), None, None),
            P(("dp", "seq"), None, None),
            P(("dp", "seq"), None, None),
        ),
        out_specs=(
            P("dp", "seq", None),
            P("dp"),
            P(("dp", "seq"), None, None),
            P(("dp", "seq"), None, None),
            P(("dp", "seq"), None, None),
        ),
        check_vma=False,
    )
```
